512 devices in a mesh: panel: 8 (over x_lo, y), gx: 64 (over z, x_hi, core).
Axes of the slice: x: 4 (x_hi: 2, x_lo: 2; x = x_hi * 2 + x_lo), y: 4, z: 16, core: 2. Of those that a mesh axis runs over, the one named last changes fastest.
Arguments:
- right_side: float32 [20, 4096, 1024], P(None, 'gx', 'panel'), may hold values from -40 to 40
- previous: float32 [20, 4096, 1024], P(None, 'gx', 'panel'), may hold values from -1.8 to 1.8
- diagonal: float32 [20, 4096, 1024], P(None, 'gx', 'panel'), may hold values from 0.5 to 2
- vertical: float32 [19, 4096, 1024], P(None, 'gx', 'panel'), may hold values from 0.5 to 2
- metric_a: float32 [4096, 1024], P('gx', 'panel'), may hold values from 0.5 to 2
- metric_b: float32 [4096, 1024], P('gx', 'panel'), may hold values from 0.5 to 2
- profile: float32 [20], replicated, may hold values from 0.5 to 2
- column_inverse: bfloat16 [4, 20, 4096, 1024], P(None, None, 'gx', 'panel'), may hold values from -0.125 to 0.625, as said below
- edge_turn: int32 [4, 64, 8], replicated, may hold values from 0 to 3
Outputs:
- increment: float32 [20, 4096, 1024], P(None, 'gx', 'panel')
The draws below stay inside these ranges and needn't reach their ends.
Inputs may be any that keep to these rules, and one draw needn't show every extreme that they name: Entry column_inverse[c, k] lies in row k mod 4, column c of the inverse of the block of 4 levels that holds level k. `edge_turn`: entries 0 and 2 are read only for their lowest bit; entries 1 and 3 reverse with the lowest bit and negate with the value 2 bit.
All inputs are finite; a program needn't handle non-finite values.
Results may differ from the reference program's by a relative error of at most 0.0003.
Values sent between devices are 32-bit elements; how exact they have to be, the bound alone decides.
No kernel may reach another device: no remote copies, remote signals or barrier semaphores. Data moves between devices by JAX's collectives and lax.ppermute only.
A program may use at most 64 MiB of HBM per device.

```python
import math
import jax
import jax.numpy as jnp

LEVELS = 20
BK = 4
TA = 64
TB = 128
NA = 4096
NB = 1024
N_PANEL = 8
N_GX = 64


def draw_right_side(key, part):
    key_rough = jax.random.fold_in(key, 0)
    ramp = 1.0 + 2.0 * jnp.arange(NA, dtype=jnp.float32)[None, :, None] / NA
    rough = jnp.clip(jax.random.normal(key_rough, (LEVELS, NA, NB), jnp.float32), -6.0, 6.0)
    return rough * ramp


def draw_column_inverse(key, part):
    key_diag, key_off = jax.random.split(key)
    full_shape = (BK, LEVELS, NA, NB)
    within = jnp.arange(LEVELS) % BK
    on_diag = (jnp.arange(BK)[:, None] == within[None, :])[:, :, None, None]
    diag_part = 0.2 * jnp.exp(jnp.log(3.0) * jax.random.uniform(key_diag, full_shape, jnp.float32))
    off_part = jax.random.uniform(key_off, full_shape, jnp.float32, -0.12, 0.12)
    return jnp.where(on_diag, diag_part, off_part).astype(jnp.bfloat16)


def with_ends(values, key, least, top_value):
    spot = [jax.random.randint(jax.random.fold_in(key, axis), (), 0, length) for axis, length in enumerate(values.shape)]
    longest = values.shape.index(max(values.shape))
    beside = spot[:longest] + [(spot[longest] + 1) % values.shape[longest]] + spot[longest + 1:]
    return values.at[tuple(spot)].set(least).at[tuple(beside)].set(top_value)


def block_scale(rng, extent, cuts, smallest, top_value):
    factor_of = 1.0
    for axis_at, shards_of in cuts:
        heights = jax.random.uniform(jax.random.fold_in(jax.random.fold_in(rng, 6), axis_at), (shards_of,), jnp.float32, smallest / len(cuts), top_value / len(cuts))
        factor_of = factor_of * jnp.repeat(jnp.exp(heights), extent[axis_at] // shards_of).reshape((-1,) + (1,) * (len(extent) - 1 - axis_at))
    return factor_of


def bell_draw(stream_key, shape, deviation, bound, shards=(), held_as=jnp.bfloat16):
    drawn = jax.random.normal(stream_key, shape, jnp.float32) * deviation
    if len(shards) > 0:
        drawn = block_scale(stream_key, shape, shards, -0.22, 0.18) * drawn
    return jnp.clip(drawn, min=-bound, max=bound).astype(held_as)


def setup_inputs(seed: int = 0) -> dict:
    arg_keys = jax.random.split(jax.random.key(seed), 10)
    right_side = draw_right_side(jax.random.fold_in(arg_keys[9], 71), 0)
    previous = bell_draw(arg_keys[1], (LEVELS, NA, NB), 0.3, 1.8, ((1, 64), (2, 8)), jnp.float32)
    diagonal = jnp.clip(jnp.exp(math.log(2.0) - 1.3862944 * jax.random.uniform(arg_keys[2], (LEVELS, NA, NB), jnp.float32) ** block_scale(arg_keys[2], (LEVELS, NA, NB), ((1, 64), (2, 8)), -0.2, 0.2)), 0.5, 2.0)
    vertical = jnp.clip(jnp.exp(math.log(2.0) - 1.3862944 * jax.random.uniform(arg_keys[3], (LEVELS - 1, NA, NB), jnp.float32) ** block_scale(arg_keys[3], (LEVELS - 1, NA, NB), ((1, 64), (2, 8)), -0.2, 0.2)), 0.5, 2.0)
    metric_a = jnp.clip(jnp.exp(math.log(2.0) - 1.3862944 * jax.random.uniform(arg_keys[4], (NA, NB), jnp.float32) ** block_scale(arg_keys[4], (NA, NB), ((0, 64), (1, 8)), -0.2, 0.2)), 0.5, 2.0)
    metric_b = jnp.clip(jnp.exp(math.log(2.0) - 1.3862944 * jax.random.uniform(arg_keys[5], (NA, NB), jnp.float32) ** block_scale(arg_keys[5], (NA, NB), ((0, 64), (1, 8)), -0.2, 0.2)), 0.5, 2.0)
    profile = jnp.clip(jnp.exp(jax.random.uniform(arg_keys[6], (LEVELS,), jnp.float32, math.log(0.5), math.log(2.0))), 0.5, 2.0)
    column_inverse = draw_column_inverse(jax.random.fold_in(arg_keys[9], 71), 0)
    edge_turn = with_ends(jax.random.randint(arg_keys[8], (4, N_GX, N_PANEL), 0, 4), jax.random.fold_in(arg_keys[8], 1), 0, 3).astype(jnp.int32)
    return dict(right_side=right_side, previous=previous, diagonal=diagonal, vertical=vertical, metric_a=metric_a, metric_b=metric_b, profile=profile, column_inverse=column_inverse, edge_turn=edge_turn)


def flip_where(condition, values, dimension):
    return jnp.where(condition, jnp.flip(values, dimension), values)


def apply_operator(pressure, diagonal, vertical, face_a, face_b, edge_turn):
    tiles = pressure.reshape(LEVELS, N_GX, TA, N_PANEL, TB)
    low_a = jnp.roll(tiles[:, :, -1], 1, axis=1)
    low_a = flip_where((edge_turn[0] % 2 == 1)[None, :, :, None], low_a, 3)
    prev_a = jnp.concatenate([low_a[:, :, None], tiles[:, :, :-1]], axis=2)
    low_b = jnp.roll(tiles[..., -1], 1, axis=3)
    low_b = flip_where((edge_turn[2] % 2 == 1)[None, :, None, :], low_b, 2)
    prev_b = jnp.concatenate([low_b[..., None], tiles[..., :-1]], axis=4)
    flux_a = face_a * (tiles - prev_a)
    flux_b = face_b * (tiles - prev_b)
    high_a = jnp.roll(flux_a[:, :, 0], -1, axis=1)
    turn_a = edge_turn[1][None, :, :, None]
    high_a = flip_where(turn_a % 2 == 1, high_a, 3)
    high_a = jnp.where(turn_a // 2 == 1, -high_a, high_a)
    next_a = jnp.concatenate([flux_a[:, :, 1:], high_a[:, :, None]], axis=2)
    high_b = jnp.roll(flux_b[..., 0], -1, axis=3)
    turn_b = edge_turn[3][None, :, None, :]
    high_b = flip_where(turn_b % 2 == 1, high_b, 2)
    high_b = jnp.where(turn_b // 2 == 1, -high_b, high_b)
    next_b = jnp.concatenate([flux_b[..., 1:], high_b[..., None]], axis=4)
    horizontal = (flux_a - next_a + flux_b - next_b).reshape(LEVELS, NA, NB)
    vertical_flux = vertical * (pressure[1:] - pressure[:-1])
    zeros_row = jnp.zeros((1, NA, NB), jnp.float32)
    upward = jnp.concatenate([zeros_row, vertical_flux], axis=0) - jnp.concatenate([vertical_flux, zeros_row], axis=0)
    return diagonal * pressure + horizontal + upward


def precondition(resid, column_inverse):
    blocks = resid.reshape(LEVELS // BK, BK, NA, NB)
    inverse = column_inverse.astype(jnp.float32).reshape(BK, LEVELS // BK, BK, NA, NB)
    result = inverse[0] * blocks[:, 0:1]
    for column in range(1, BK):
        result = result + inverse[column] * blocks[:, column:column + 1]
    return result.reshape(LEVELS, NA, NB)


def reference(right_side, previous, diagonal, vertical, metric_a, metric_b, profile, column_inverse, edge_turn):
    face_a = (metric_a[None] * profile[:, None, None]).reshape(LEVELS, N_GX, TA, N_PANEL, TB)
    face_b = (metric_b[None] * profile[:, None, None]).reshape(LEVELS, N_GX, TA, N_PANEL, TB)

    def operate(values):
        return apply_operator(values, diagonal, vertical, face_a, face_b, edge_turn)

    resid_first = right_side - operate(previous)
    search_first = precondition(resid_first, column_inverse)
    image_first = operate(search_first)
    square_first = jnp.sum(image_first * image_first)
    alpha_first = jnp.sum(resid_first * image_first) / square_first
    resid_second = resid_first - alpha_first * image_first
    search_second = precondition(resid_second, column_inverse)
    image_second = operate(search_second)
    beta_coef = jnp.sum(image_second * image_first) / square_first
    direction = search_second - beta_coef * search_first
    image_final = image_second - beta_coef * image_first
    alpha_second = jnp.sum(resid_second * image_final) / jnp.sum(image_final * image_final)
    return alpha_first * search_first + alpha_second * direction
```

```python
import jax
import jax.numpy as jnp
from jax import lax
from jax.experimental import pallas as pl
from jax.experimental.pallas import tpu as pltpu
from jax.sharding import Mesh
from jax.sharding import PartitionSpec as P

BK = 4
SHAPE = (2, 4, 16, 2, 2)
GX = ("gx_0", "gx_1", "gx_2")
PANEL = ("panel_0", "panel_1")
PLANE = ("panel_0", "panel_1", "gx_1", "gx_2")
COLUMN = ("gx_0",)
ROWS = 24
METRIC = 20
F32 = jnp.float32
VMEM = pl.BlockSpec(memory_space=pltpu.VMEM)


def reverse_lanes(values, length):
    lane = lax.broadcasted_iota(jnp.int32, values.shape, 1)
    index = jnp.where(lane < length, length - 1 - lane, lane)
    return jnp.take_along_axis(values, index, axis=1)


def reverse_rows(values):
    count = values.shape[0] // 8
    row = lax.broadcasted_iota(jnp.int32, (8, 128), 0)
    parts = [
        jnp.take_along_axis(values[8 * i : 8 * i + 8], 7 - row, axis=0)
        for i in reversed(range(count))
    ]
    return jnp.concatenate(parts, axis=0)


def flag(flags_ref, at):
    return flags_ref[at : at + 1, :]


def pack(field_ref, flags_ref, row_up, row_down, col_up, col_down, metrics=None):
    levels, height, width = field_ref.shape
    lane = lax.broadcasted_iota(jnp.int32, (height, width), 1)
    for k in range(levels):
        row_up[k : k + 1, :] = field_ref[k, height - 1 : height, :]
        row_down[k : k + 1, :] = field_ref[k, 0:1, :]
    for k in range(levels, ROWS):
        row_up[k : k + 1, :] = jnp.zeros((1, width), F32)
        row_down[k : k + 1, :] = jnp.zeros((1, width), F32)
    last = jnp.zeros((height, width), F32)
    first = jnp.zeros((height, width), F32)
    for k in range(levels):
        values = field_ref[k]
        last = jnp.where(lane == k, pltpu.roll(values, (k + 1) % width, 1), last)
        first = jnp.where(lane == k, pltpu.roll(values, k, 1) if k else values, first)
    if metrics is not None:
        metric_a, metric_b = metrics
        row_down[METRIC : METRIC + 1, :] = metric_a[0:1, :]
        first = jnp.where(lane == METRIC, pltpu.roll(metric_b[...], METRIC, 1), first)
    up, down = row_up[...], row_down[...]
    row_up[...] = jnp.where(flag(flags_ref, 0) > 0.5, reverse_lanes(up, width), up)
    row_down[...] = jnp.where(flag(flags_ref, 1) > 0.5, reverse_lanes(down, width), down)
    col_up[...] = jnp.where(flag(flags_ref, 2) > 0.5, reverse_rows(last), last)
    col_down[...] = jnp.where(flag(flags_ref, 3) > 0.5, reverse_rows(first), first)


def apply_operator(field_ref, coef, halo, flux_ref, emit):
    diagonal, vertical, metric_a, metric_b, spread, lanes, flags_ref = coef
    low_row, high_row, low_col, high_col, sent_row, sent_col, metric_row, metric_col = halo
    levels, height, width = field_ref.shape
    row = lax.broadcasted_iota(jnp.int32, (height, width), 0)
    lane = lax.broadcasted_iota(jnp.int32, (height, width), 1)
    own_row = sent_row[...]
    own_row = jnp.where(flag(flags_ref, 4) > 0.5, reverse_lanes(own_row, width), own_row)
    face_row = metric_row[METRIC : METRIC + 1, :] * spread[...]
    flux_ref[...] = flag(flags_ref, 5) * (face_row * (high_row[...] - own_row))
    own_col = sent_col[...]
    own_col = jnp.where(flag(flags_ref, 6) > 0.5, reverse_rows(own_col), own_col)
    face_col = metric_col[:, METRIC : METRIC + 1] * lanes[0:1, :]
    flux_col = flag(flags_ref, 7) * (face_col * (high_col[...] - own_col))
    below = None
    for k in range(levels):
        here = field_ref[k]
        scale = spread[k : k + 1, :]
        face_a = metric_a[...] * scale
        face_b = metric_b[...] * scale
        prev_a = jnp.where(row == 0, low_row[k : k + 1, :], pltpu.roll(here, 1, 0))
        edge = low_col[...]
        edge = pltpu.roll(edge, width - k, 1) if k else edge
        prev_b = jnp.where(lane == 0, edge, pltpu.roll(here, 1, 1))
        flux_a = face_a * (here - prev_a)
        flux_b = face_b * (here - prev_b)
        next_a = jnp.where(
            row == height - 1, flux_ref[k : k + 1, :], pltpu.roll(flux_a, height - 1, 0)
        )
        next_b = jnp.where(
            lane == width - 1,
            pltpu.roll(flux_col, width - 1 - k, 1),
            pltpu.roll(flux_b, width - 1, 1),
        )
        total = diagonal[k] * here + (flux_a - next_a + flux_b - next_b)
        if k + 1 < levels:
            above = vertical[k] * (field_ref[k + 1] - here)
            total = total + ((below - above) if k else -above)
            below = above
        else:
            total = total + below
        emit(k, total)


def precondition(resid_ref, inverse_ref, out_ref):
    levels, height, _ = resid_ref.shape
    step = 16
    for block in range(0, levels, BK):
        for at in range(0, height, step):
            rows = slice(at, at + step)
            resid = [resid_ref[block + c, rows, :] for c in range(BK)]
            for k in range(block, block + BK):
                total = inverse_ref[0, k, rows, :].astype(F32) * resid[0]
                for c in range(1, BK):
                    total = total + inverse_ref[c, k, rows, :].astype(F32) * resid[c]
                out_ref[k, rows, :] = total


def by_sublane(values):
    total = values[0:8]
    for at in range(8, values.shape[0], 8):
        total = total + values[at : at + 8]
    return total


def pack_kernel(where_ref, turn_ref, field, metric_a, metric_b, flags, row_up, row_down, col_up, col_down):
    gx, panel = where_ref[0], where_ref[1]
    n_panel, n_gx = turn_ref.shape[1:]
    q = lax.broadcasted_iota(jnp.int32, (n_panel, n_gx), 0)
    g = lax.broadcasted_iota(jnp.int32, (n_panel, n_gx), 1)

    def at(edge, dg, dq):
        gg = lax.rem(gx + dg + n_gx, n_gx)
        qq = lax.rem(panel + dq + n_panel, n_panel)
        picked = jnp.where((g == gg) & (q == qq), turn_ref[edge], 0).astype(F32)
        return jnp.sum(jnp.sum(picked, axis=1, keepdims=True), axis=0, keepdims=True)

    def odd(code):
        return jnp.where((code == 1.0) | (code == 3.0), 1.0, 0.0)

    def sign(code):
        return jnp.where(code >= 2.0, -1.0, 1.0)

    own_a, own_b = at(1, 0, 0), at(3, 0, 0)
    found = (
        odd(at(0, 1, 0)), odd(at(1, -1, 0)), odd(at(2, 0, 1)), odd(at(3, 0, -1)),
        odd(own_a), sign(own_a), odd(own_b), sign(own_b),
    )
    for i, value in enumerate(found):
        flags[i : i + 1, :] = jnp.broadcast_to(value, (1, 128))
    pack(field, flags, row_up, row_down, col_up, col_down, (metric_a, metric_b))


def first_kernel(field, right_side, inverse, *refs):
    coef, halo, (resid, search, *edges), (flux,) = refs[:7], refs[7:15], refs[15:21], refs[21:]

    def emit(k, image):
        resid[k] = right_side[k] - image

    apply_operator(field, coef, halo, flux, emit)
    precondition(resid, inverse, search)
    pack(search, coef[6], *edges)


def second_kernel(field, resid, inverse, *refs):
    coef, halo, (image, search, sums, *edges), (flux,) = refs[:7], refs[7:15], refs[15:22], refs[22:]
    totals = [jnp.zeros((8, 128), F32) for _ in range(2)]

    def emit(k, value):
        image[k] = value
        totals[0] = totals[0] + by_sublane(resid[k] * value)
        totals[1] = totals[1] + by_sublane(value * value)

    apply_operator(field, coef, halo, flux, emit)
    for i, total in enumerate(totals):
        sums[i : i + 1, :] = jnp.sum(total, axis=0, keepdims=True)
    sums[2:, :] = jnp.zeros((6, 128), F32)
    precondition(image, inverse, search)
    pack(search, coef[6], *edges)


def third_kernel(field, resid, first, sums_in, *refs):
    coef, halo, (sums,), (flux,) = refs[:7], refs[7:15], refs[15:16], refs[16:]
    totals = [jnp.zeros((8, 128), F32) for _ in range(3)]

    def emit(k, value):
        totals[0] = totals[0] + by_sublane(first[k] * value)
        totals[1] = totals[1] + by_sublane(value * value)
        totals[2] = totals[2] + by_sublane(resid[k] * value)

    apply_operator(field, coef, halo, flux, emit)
    row = lax.broadcasted_iota(jnp.int32, (8, 128), 0)
    packed = sums_in[...]
    for i, total in enumerate(totals):
        packed = jnp.where(row == 2 + i, jnp.sum(total, axis=0, keepdims=True), packed)
    for i in range(sums.shape[0]):
        sums[i] = packed


def last_kernel(parts, first, second, out):
    total = parts[0]
    for i in range(1, parts.shape[0]):
        total = total + parts[i]
    total = jnp.sum(total, axis=1, keepdims=True)
    cross1, square1, along, square2, cross2 = (total[i : i + 1, :] for i in range(5))
    alpha = cross1 / square1
    ratio = along / square1
    weight2 = (cross2 - ratio * cross1) / (square2 - ratio * along)
    weight1 = alpha - ratio * weight2
    for k in range(first.shape[0]):
        out[k] = weight1 * first[k] + weight2 * second[k]


def call(body, operands, outs, scratch=(), smem=0, flops=1 << 22):
    specs = [pl.BlockSpec(memory_space=pltpu.SMEM)] * smem + [VMEM] * (len(operands) - smem)
    return pl.pallas_call(
        body,
        out_shape=tuple(jax.ShapeDtypeStruct(shape, F32) for shape in outs),
        in_specs=specs,
        out_specs=tuple(VMEM for _ in outs),
        scratch_shapes=tuple(pltpu.VMEM(shape, F32) for shape in scratch),
        compiler_params=pltpu.CompilerParams(vmem_limit_bytes=16 << 20),
        cost_estimate=pl.CostEstimate(flops=flops, bytes_accessed=1 << 20, transcendentals=0),
    )(*operands)


def shift(block, axis, distance):
    count = lax.axis_size(axis)
    return lax.ppermute(block, axis, [((i - distance) % count, i) for i in range(count)])


def exchange(row_up, row_down, col_up, col_down):
    low_row = shift(row_up, GX, 1)
    low_col = shift(col_up, PANEL, 1)
    high_row = shift(row_down, GX, -1)
    high_col = shift(col_down, PANEL, -1)
    return low_row, high_row, low_col, high_col


def sum_over(parts, axes):
    return lax.all_to_all(parts, axes, 0, 0, tiled=True)


def shards(
    right_side, previous, diagonal, vertical, metric_a, metric_b, profile, column_inverse, edge_turn
):
    levels, height, width = right_side.shape
    place = jnp.stack([lax.axis_index(GX), lax.axis_index(PANEL)]).astype(jnp.int32)
    spread = jnp.broadcast_to(jnp.pad(profile, (0, ROWS - levels))[:, None], (ROWS, width))
    lanes = jnp.broadcast_to(jnp.pad(profile, (0, width - levels))[None], (8, width))
    row, col, field, sums = (ROWS, width), (height, width), right_side.shape, (8, width)
    edges = [row, row, col, col]

    flags, *sent = call(
        pack_kernel,
        (place, jnp.transpose(edge_turn, (0, 2, 1)), previous, metric_a, metric_b),
        [(8, width), *edges],
        smem=1,
    )
    coef = (diagonal, vertical, metric_a, metric_b, spread, lanes, flags)
    halo = exchange(*sent)
    metrics = (halo[1], halo[3])
    resid, search_first, *sent1 = call(
        first_kernel,
        (previous, right_side, column_inverse, *coef, *halo, sent[0], sent[2], *metrics),
        [field, field, *edges],
        [row],
    )
    halo = exchange(*sent1)
    image_first, search_next, part, *sent2 = call(
        second_kernel,
        (search_first, resid, column_inverse, *coef, *halo, sent1[0], sent1[2], *metrics),
        [field, field, sums, *edges],
        [row],
    )
    halo = exchange(*sent2)
    plane = lax.axis_size(PLANE)
    depth = lax.axis_size(COLUMN)
    (parts,) = call(
        third_kernel,
        (search_next, resid, image_first, part, *coef, *halo, sent2[0], sent2[2], *metrics),
        [(plane, *sums)],
        [row],
    )
    part = jnp.sum(sum_over(parts, PLANE), axis=0)
    parts = sum_over(jnp.broadcast_to(part[None], (depth, *sums)), COLUMN)
    (increment,) = call(last_kernel, (parts, search_first, search_next), [field])
    return increment


def solution(mesh):
    finer = Mesh(
        mesh.devices.reshape(SHAPE), ("panel_0", "panel_1", "gx_0", "gx_1", "gx_2")
    )
    spec = P(None, GX, PANEL)
    in_specs = (
        spec, spec, spec, spec, P(GX, PANEL), P(GX, PANEL), P(), P(None, None, GX, PANEL), P(),
    )
    return jax.shard_map(shards, mesh=finer, in_specs=in_specs, out_specs=spec, check_vma=False)
```

```python
import jax
import jax.numpy as jnp
from jax import lax
from jax.experimental import pallas as pl
from jax.experimental.pallas import tpu as pltpu
from jax.sharding import Mesh
from jax.sharding import PartitionSpec as P

BK = 4
SHAPE = (2, 4, 16, 2, 2)
GX = ("gx_0", "gx_1", "gx_2")
PANEL = ("panel_0", "panel_1")
PLANE = ("panel_0", "panel_1", "gx_1", "gx_2")
COLUMN = ("gx_0",)
ROWS = 24
LOAD_LIMIT = 16 << 20
METRIC = 20
F32 = jnp.float32
VMEM = pl.BlockSpec(memory_space=pltpu.VMEM)
HBM = pl.BlockSpec(memory_space=pltpu.HBM)


def reverse_lanes(values, length):
    lane = lax.broadcasted_iota(jnp.int32, values.shape, 1)
    index = jnp.where(lane < length, length - 1 - lane, lane)
    return jnp.take_along_axis(values, index, axis=1)


def reverse_rows(values):
    count = values.shape[0] // 8
    row = lax.broadcasted_iota(jnp.int32, (8, 128), 0)
    parts = [
        jnp.take_along_axis(values[8 * i : 8 * i + 8], 7 - row, axis=0)
        for i in reversed(range(count))
    ]
    return jnp.concatenate(parts, axis=0)


def flag(flags_ref, at):
    return flags_ref[at : at + 1, :]


def pack(field_ref, flags_ref, row_ref, edges, metrics=None):
    up_ref, down_ref = row_ref
    row_near, row_far, col_near, col_far = edges
    levels, height, width = field_ref.shape
    lane = lax.broadcasted_iota(jnp.int32, (height, width), 1)
    for k in range(levels):
        up_ref[k : k + 1, :] = field_ref[k, height - 1 : height, :]
        down_ref[k : k + 1, :] = field_ref[k, 0:1, :]
    for k in range(levels, ROWS):
        up_ref[k : k + 1, :] = jnp.zeros((1, width), F32)
        down_ref[k : k + 1, :] = jnp.zeros((1, width), F32)
    last = jnp.zeros((height, width), F32)
    first = jnp.zeros((height, width), F32)
    for k in range(levels):
        values = field_ref[k]
        last = jnp.where(lane == k, pltpu.roll(values, (k + 1) % width, 1), last)
        first = jnp.where(lane == k, pltpu.roll(values, k, 1) if k else values, first)
    if metrics is not None:
        metric_a, metric_b = metrics
        down_ref[METRIC : METRIC + 1, :] = metric_a[0:1, :]
        first = jnp.where(lane == METRIC, pltpu.roll(metric_b[...], METRIC, 1), first)
    up, down = up_ref[...], down_ref[...]
    up = jnp.where(flag(flags_ref, 0) > 0.5, reverse_lanes(up, width), up)
    down = jnp.where(flag(flags_ref, 1) > 0.5, reverse_lanes(down, width), down)
    last = jnp.where(flag(flags_ref, 2) > 0.5, reverse_rows(last), last)
    first = jnp.where(flag(flags_ref, 3) > 0.5, reverse_rows(first), first)
    even_a, even_b = flag(flags_ref, 8) > 0.5, flag(flags_ref, 9) > 0.5
    row_near[...] = jnp.where(even_a, up, down)
    row_far[...] = jnp.where(even_a, down, up)
    col_near[...] = jnp.where(even_b, last, first)
    col_far[...] = jnp.where(even_b, first, last)


def neighbours(flags_ref, got, sent):
    even_a, even_b = flag(flags_ref, 8) > 0.5, flag(flags_ref, 9) > 0.5
    row_near, row_far, col_near, col_far = (ref[...] for ref in got)
    own_near, own_far, mine_near, mine_far = (ref[...] for ref in sent)
    return (
        jnp.where(even_a, row_far, row_near), jnp.where(even_a, row_near, row_far),
        jnp.where(even_b, col_far, col_near), jnp.where(even_b, col_near, col_far),
        jnp.where(even_a, own_near, own_far), jnp.where(even_b, mine_near, mine_far),
    )


def apply_operator(field_ref, coef, near, faces, scratch, emit):
    diagonal, vertical, metric_a, metric_b, spread, _, flags_ref = coef
    low, high_row, low_col, high_col, own_row, own_col = near
    face_row, face_col = faces
    low_row, flux_ref = scratch
    levels, height, width = field_ref.shape
    row = lax.broadcasted_iota(jnp.int32, (height, width), 0)
    lane = lax.broadcasted_iota(jnp.int32, (height, width), 1)
    low_row[...] = low
    own_row = jnp.where(flag(flags_ref, 4) > 0.5, reverse_lanes(own_row, width), own_row)
    flux_ref[...] = flag(flags_ref, 5) * (face_row * (high_row - own_row))
    own_col = jnp.where(flag(flags_ref, 6) > 0.5, reverse_rows(own_col), own_col)
    flux_col = flag(flags_ref, 7) * (face_col * (high_col - own_col))
    below = None
    for k in range(levels):
        here = field_ref[k]
        scale = spread[k : k + 1, :]
        face_a = metric_a[...] * scale
        face_b = metric_b[...] * scale
        prev_a = jnp.where(row == 0, low_row[k : k + 1, :], pltpu.roll(here, 1, 0))
        edge = pltpu.roll(low_col, width - k, 1) if k else low_col
        prev_b = jnp.where(lane == 0, edge, pltpu.roll(here, 1, 1))
        flux_a = face_a * (here - prev_a)
        flux_b = face_b * (here - prev_b)
        next_a = jnp.where(
            row == height - 1, flux_ref[k : k + 1, :], pltpu.roll(flux_a, height - 1, 0)
        )
        next_b = jnp.where(
            lane == width - 1,
            pltpu.roll(flux_col, width - 1 - k, 1),
            pltpu.roll(flux_b, width - 1, 1),
        )
        total = diagonal[k] * here + (flux_a - next_a + flux_b - next_b)
        if k + 1 < levels:
            above = vertical[k] * (field_ref[k + 1] - here)
            total = total + ((below - above) if k else -above)
            below = above
        else:
            total = total + below
        emit(k, total)


def precondition(resid_ref, inverse_ref, out_ref):
    levels, height, _ = resid_ref.shape
    step = 16
    for block in range(0, levels, BK):
        for at in range(0, height, step):
            rows = slice(at, at + step)
            resid = [resid_ref[block + c, rows, :] for c in range(BK)]
            for k in range(block, block + BK):
                total = inverse_ref[0, k, rows, :].astype(F32) * resid[0]
                for c in range(1, BK):
                    total = total + inverse_ref[c, k, rows, :].astype(F32) * resid[c]
                out_ref[k, rows, :] = total


def by_sublane(values):
    total = values[0:8]
    for at in range(8, values.shape[0], 8):
        total = total + values[at : at + 8]
    return total


def load_kernel(turn, profile, *refs):
    sources, outs, scratch = refs[:7], refs[7:21], refs[21:]
    copies_to, (spread, lanes, flags), edges = outs[:7], outs[7:10], outs[10:]
    turn_ref, profile_ref, up_ref, down_ref, sems = scratch
    pairs = [(turn, turn_ref), (profile, profile_ref), *zip(sources, copies_to)]
    copies = [pltpu.make_async_copy(a, b, sems.at[i]) for i, (a, b) in enumerate(pairs)]
    for copy in copies:
        copy.start()
    gx, panel = lax.axis_index(GX), lax.axis_index(PANEL)
    n_panel, n_gx = turn.shape[1:]
    q = lax.broadcasted_iota(jnp.int32, (n_panel, n_gx), 0)
    g = lax.broadcasted_iota(jnp.int32, (n_panel, n_gx), 1)
    copies[0].wait()

    def at(edge, dg, dq):
        gg = lax.rem(gx + dg + n_gx, n_gx)
        qq = lax.rem(panel + dq + n_panel, n_panel)
        picked = jnp.where((g == gg) & (q == qq), turn_ref[edge], 0).astype(F32)
        return jnp.sum(jnp.sum(picked, axis=1, keepdims=True), axis=0, keepdims=True)

    def odd(code):
        return jnp.where((code == 1.0) | (code == 3.0), 1.0, 0.0)

    def sign(code):
        return jnp.where(code >= 2.0, -1.0, 1.0)

    def even(place):
        return jnp.full((1, 128), 1 - lax.rem(place, 2), jnp.int32).astype(F32)

    own_a, own_b = at(1, 0, 0), at(3, 0, 0)
    found = (
        odd(at(0, 1, 0)), odd(at(1, -1, 0)), odd(at(2, 0, 1)), odd(at(3, 0, -1)),
        odd(own_a), sign(own_a), odd(own_b), sign(own_b), even(gx), even(panel),
    )
    for i, value in enumerate(found):
        flags[i : i + 1, :] = jnp.broadcast_to(value, (1, 128))
    copies[1].wait()
    levels = sources[0].shape[0]
    lane = lax.broadcasted_iota(jnp.int32, lanes.shape, 1)
    in_lanes = jnp.zeros(lanes.shape, F32)
    for k in range(levels):
        spread[k : k + 1, :] = jnp.full((1, spread.shape[1]), profile_ref[k], F32)
        in_lanes = jnp.where(lane == k, profile_ref[k], in_lanes)
    spread[levels:, :] = jnp.zeros((ROWS - levels, spread.shape[1]), F32)
    lanes[...] = in_lanes
    for copy in copies[2:5]:
        copy.wait()
    pack(copies_to[0], flags, (up_ref, down_ref), edges, copies_to[1:3])
    for copy in copies[5:]:
        copy.wait()


def first_kernel(field, right_side, inverse, *refs):
    coef, got, sent, outs, scratch = refs[:7], refs[7:11], refs[11:15], refs[15:23], refs[23:]
    (resid, search, face_row, face_col), edges = outs[:4], outs[4:]
    near = neighbours(coef[6], got, sent)
    face_row[...] = near[1][METRIC : METRIC + 1, :] * coef[4][...]
    face_col[...] = near[3][:, METRIC : METRIC + 1] * coef[5][0:1, :]

    def emit(k, image):
        resid[k] = right_side[k] - image

    apply_operator(field, coef, near, (face_row[...], face_col[...]), scratch, emit)
    precondition(resid, inverse, search)
    pack(search, coef[6], scratch, edges)


def second_kernel(field, resid, inverse, face_row, face_col, *refs):
    coef, got, sent, outs, scratch = refs[:7], refs[7:11], refs[11:15], refs[15:22], refs[22:]
    (image, search, sums), edges = outs[:3], outs[3:]
    totals = [jnp.zeros((8, 128), F32) for _ in range(2)]

    def emit(k, value):
        image[k] = value
        totals[0] = totals[0] + by_sublane(resid[k] * value)
        totals[1] = totals[1] + by_sublane(value * value)

    near = neighbours(coef[6], got, sent)
    apply_operator(field, coef, near, (face_row[...], face_col[...]), scratch, emit)
    for i, total in enumerate(totals):
        sums[i] = total
    precondition(image, inverse, search)
    pack(search, coef[6], scratch, edges)


def third_kernel(field, resid, first, sums, face_row, face_col, *refs):
    coef, got, sent, (out,), scratch = refs[:7], refs[7:11], refs[11:15], refs[15:16], refs[16:]
    totals = [jnp.zeros((8, 128), F32) for _ in range(3)]

    def emit(k, value):
        totals[0] = totals[0] + by_sublane(first[k] * value)
        totals[1] = totals[1] + by_sublane(value * value)
        totals[2] = totals[2] + by_sublane(resid[k] * value)

    near = neighbours(coef[6], got, sent)
    apply_operator(field, coef, near, (face_row[...], face_col[...]), scratch, emit)
    row = lax.broadcasted_iota(jnp.int32, (8, 128), 0)
    lane = lax.broadcasted_iota(jnp.int32, (8, 128), 1)
    packed = jnp.zeros((8, 128), F32)
    for i, total in enumerate([sums[0], sums[1], *totals]):
        packed = jnp.where(row == i, jnp.sum(total, axis=0, keepdims=True), packed)
    packed = jnp.where(row == lane, jnp.sum(packed, axis=1, keepdims=True), 0.0)
    packed = jnp.sum(packed, axis=0, keepdims=True)
    for i in range(out.shape[0]):
        out[i] = packed


def last_kernel(parts, first, second, out):
    total = parts[0]
    for i in range(1, parts.shape[0]):
        total = total + parts[i]
    cross1, square1, along, square2, cross2 = (total[:, i : i + 1] for i in range(5))
    alpha = cross1 / square1
    ratio = along / square1
    weight2 = (cross2 - ratio * cross1) / (square2 - ratio * along)
    weight1 = alpha - ratio * weight2
    for k in range(first.shape[0]):
        out[k] = weight1 * first[k] + weight2 * second[k]


def call(body, operands, outs, scratch=(), specs=None, limit=16 << 20, flops=1 << 22):
    return pl.pallas_call(
        body,
        out_shape=tuple(
            jax.ShapeDtypeStruct(out.shape, out.dtype) if hasattr(out, "dtype") else
            jax.ShapeDtypeStruct(out, F32) for out in outs
        ),
        in_specs=specs or [VMEM] * len(operands),
        out_specs=tuple(VMEM for _ in outs),
        scratch_shapes=tuple(
            pltpu.VMEM(shape, F32) if isinstance(shape, tuple) else shape for shape in scratch
        ),
        compiler_params=pltpu.CompilerParams(vmem_limit_bytes=limit),
        cost_estimate=pl.CostEstimate(flops=flops, bytes_accessed=1 << 20, transcendentals=0),
    )(*operands)


def swap(block, axis, offset):
    count = lax.axis_size(axis)
    pairs = []
    for low in range(offset, count + offset, 2):
        high = (low + 1) % count
        pairs += [(low, high), (high, low)]
    return lax.ppermute(block, axis, pairs)


def exchange(row_near, row_far, col_near, col_far):
    row_far = swap(row_far, GX, 1)
    col_far = swap(col_far, PANEL, 1)
    col_near = swap(col_near, PANEL, 0)
    row_near = swap(row_near, GX, 0)
    return row_near, row_far, col_near, col_far


def sum_over(parts, axes):
    return lax.all_to_all(parts, axes, 0, 0, tiled=True)


def shards(
    right_side, previous, diagonal, vertical, metric_a, metric_b, profile, column_inverse, edge_turn
):
    _, height, width = right_side.shape
    row, col, field = (ROWS, width), (height, width), right_side.shape
    edges = [row, row, col, col]
    turns = jnp.transpose(edge_turn, (0, 2, 1))
    sources = (previous, metric_a, metric_b, diagonal, vertical, right_side, column_inverse)
    loaded = call(
        load_kernel,
        [pltpu.with_memory_space_constraint(x, pltpu.HBM) for x in (turns, profile, *sources)],
        [*sources, row, (8, width), (16, width), *edges],
        [
            pltpu.VMEM(turns.shape, jnp.int32), pltpu.SMEM(profile.shape, F32), row, row,
            pltpu.SemaphoreType.DMA((9,)),
        ],
        specs=[HBM] * 9,
        limit=LOAD_LIMIT,
    )
    previous, metric_a, metric_b, diagonal, vertical, right_side, column_inverse = loaded[:7]
    spread, lanes, flags, *sent = loaded[7:]
    coef = (diagonal, vertical, metric_a, metric_b, spread, lanes, flags)
    got = exchange(*sent)
    resid, search_first, *faces, e0, e1, e2, e3 = call(
        first_kernel,
        (previous, right_side, column_inverse, *coef, *got, *sent),
        [field, field, row, col, *edges],
        [row, row],
    )
    sent = (e0, e1, e2, e3)
    got = exchange(*sent)
    image_first, search_next, part, *sent2 = call(
        second_kernel,
        (search_first, resid, column_inverse, *faces, *coef, *got, *sent),
        [field, field, (2, 8, width), *edges],
        [row, row],
    )
    got = exchange(*sent2)
    plane = lax.axis_size(PLANE)
    depth = lax.axis_size(COLUMN)
    (parts,) = call(
        third_kernel,
        (search_next, resid, image_first, part, *faces, *coef, *got, *sent2),
        [(plane, 1, width)],
        [row, row],
    )
    part = jnp.sum(sum_over(parts, PLANE), axis=0)
    parts = sum_over(jnp.broadcast_to(part[None], (depth, 1, width)), COLUMN)
    (increment,) = call(last_kernel, (parts, search_first, search_next), [field])
    return increment


def solution(mesh):
    finer = Mesh(
        mesh.devices.reshape(SHAPE), ("panel_0", "panel_1", "gx_0", "gx_1", "gx_2")
    )
    spec = P(None, GX, PANEL)
    in_specs = (
        spec, spec, spec, spec, P(GX, PANEL), P(GX, PANEL), P(), P(None, None, GX, PANEL), P(),
    )
    return jax.shard_map(shards, mesh=finer, in_specs=in_specs, out_specs=spec, check_vma=False)
```
